32 devices in a mesh: batch: 4 (over z), rows: 8 (over y, x, core).
Axes of the slice: x: 2, y: 2, z: 4, core: 2. Of those that a mesh axis runs over, the one named last changes fastest.
Arguments:
- level_two: bfloat16 [8, 64, 256, 256], P('batch', 'rows'), parts along dimension 0, may hold values from -130 to 130
- level_three: bfloat16 [8, 32, 128, 512], P('batch', 'rows'), parts along dimension 0, may hold values from -130 to 130
- level_four: bfloat16 [8, 16, 64, 1024], P('batch', 'rows'), parts along dimension 0, may hold values from -130 to 130
- level_five: bfloat16 [8, 8, 32, 2048], P('batch', 'rows'), parts along dimension 0, may hold values from -130 to 130
- lateral_two: bfloat16 [256, 256], replicated, may hold values from -0.375 to 0.375
- lateral_three: bfloat16 [512, 256], replicated, may hold values from -0.25 to 0.25
- lateral_four: bfloat16 [1024, 256], replicated, may hold values from -0.1875 to 0.1875
- lateral_five: bfloat16 [2048, 256], replicated, may hold values from -0.125 to 0.125
- lateral_bias: float32 [4, 256], replicated, may hold values from -4 to 4
- smooth_weight: bfloat16 [4, 3, 768, 256], replicated, may hold values from -0.125 to 0.125
- norm_gain: float32 [4, 256], replicated, may hold values from 0.5 to 1.5
- norm_shift: float32 [4, 256], replicated, may hold values from -2 to 2
Outputs:
- pyramid_two: bfloat16 [8, 64, 256, 256], P('batch', 'rows'), parts along dimension 0
- pyramid_three: bfloat16 [8, 32, 128, 256], P('batch', 'rows'), parts along dimension 0
- pyramid_four: bfloat16 [8, 16, 64, 256], P('batch', 'rows'), parts along dimension 0
- pyramid_five: bfloat16 [8, 8, 32, 256], P('batch', 'rows'), parts along dimension 0
The draws below stay inside these ranges and needn't reach their ends.
There are 4 independent parts, one for each index of `batch`. The reference program is written for one: setup_inputs(seed, part) draws one part's arguments, and reference() takes and returns one part's arrays. A program takes and returns all parts, laid end to end along the dimension named above; an argument that names none is the same for every part. Nothing has to cross between parts.
All inputs are finite; a program needn't handle non-finite values.
Results may differ from the reference program's by a relative error of at most 0.0054.
Values may be sent and summed in bfloat16 or wider, within the bound.
No kernel may reach another device: no remote copies, remote signals or barrier semaphores. Data moves between devices by JAX's collectives and lax.ppermute only.
A program may use at most 128 MiB of HBM per device.

```python
import math
import jax
import jax.numpy as jnp
from jax import lax

CHANNELS = 256
DEPTH_TWO = 256
DEPTH_THREE = 512
DEPTH_FOUR = 1024
DEPTH_FIVE = 2048
GROUPS = 32
LEVELS = 4
IMAGES = 2
COLUMNS = 256
HEIGHT = 64


def feature_draw(key, rows_all, cols_all, depth_all, salt_code):
    base_key = jax.random.fold_in(key, salt_code)
    subkeys = jax.random.split(base_key, 3)
    relative = (jnp.arange(rows_all, dtype=jnp.float32) + 0.5) / rows_all
    jitter = jnp.exp(jax.random.uniform(subkeys[0], (IMAGES, rows_all), jnp.float32, 0.0, math.log(3.3)))
    row_scale = jnp.exp(math.log(3.0) * relative)[None, :] * jitter
    chan_scale = jnp.exp(jax.random.uniform(subkeys[1], (depth_all,), jnp.float32, -0.5 * math.log(10.0), 0.5 * math.log(10.0)))
    shape_all = (IMAGES, rows_all, cols_all, depth_all)
    values = jnp.clip(jax.random.normal(subkeys[2], shape_all, jnp.float32), -4.0, 4.0)
    return (values * row_scale[:, :, None, None] * chan_scale).astype(jnp.bfloat16)


def draw_level_two(key, part):
    return feature_draw(key, HEIGHT, COLUMNS, DEPTH_TWO, 11)


def draw_level_three(key, part):
    return feature_draw(key, HEIGHT // 2, COLUMNS // 2, DEPTH_THREE, 12)


def draw_level_four(key, part):
    return feature_draw(key, HEIGHT // 4, COLUMNS // 4, DEPTH_FOUR, 13)


def draw_level_five(key, part):
    return feature_draw(key, HEIGHT // 8, COLUMNS // 8, DEPTH_FIVE, 14)


def bell_draw(rng, shape, width, bound, kind=jnp.bfloat16):
    values = jax.random.normal(rng, shape, jnp.float32) * width
    return jnp.minimum(jnp.maximum(values, -bound), bound).astype(kind)


def setup_inputs(seed: int = 0, part: int = 0) -> dict:
    key_of = jax.random.split(jax.random.key(seed), 13)
    own_keys = jax.random.split(jax.random.fold_in(key_of[12], part), 13)
    return {
        "level_two": draw_level_two(jax.random.fold_in(jax.random.fold_in(key_of[12], part), 71), part),
        "level_three": draw_level_three(jax.random.fold_in(jax.random.fold_in(key_of[12], part), 71), part),
        "level_four": draw_level_four(jax.random.fold_in(jax.random.fold_in(key_of[12], part), 71), part),
        "level_five": draw_level_five(jax.random.fold_in(jax.random.fold_in(key_of[12], part), 71), part),
        "lateral_two": bell_draw(key_of[4], (DEPTH_TWO, CHANNELS), DEPTH_TWO ** -0.5, 0.375),
        "lateral_three": bell_draw(key_of[5], (DEPTH_THREE, CHANNELS), DEPTH_THREE ** -0.5, 0.25),
        "lateral_four": bell_draw(key_of[6], (DEPTH_FOUR, CHANNELS), DEPTH_FOUR ** -0.5, 0.1875),
        "lateral_five": bell_draw(key_of[7], (DEPTH_FIVE, CHANNELS), DEPTH_FIVE ** -0.5, 0.125),
        "lateral_bias": bell_draw(key_of[8], (LEVELS, CHANNELS), 1.0, 4.0, jnp.float32),
        "smooth_weight": bell_draw(key_of[9], (LEVELS, 3, 3 * CHANNELS, CHANNELS), (9 * CHANNELS) ** -0.5, 0.125),
        "norm_gain": jnp.clip(1.0 + 0.1 * jax.random.normal(key_of[10], (LEVELS, CHANNELS), jnp.float32), 0.5, 1.5),
        "norm_shift": bell_draw(key_of[11], (LEVELS, CHANNELS), 0.5, 2.0, jnp.float32),
    }


epsilon = 1e-05

def refine(widened, axis_pos):
    length = widened.shape[axis_pos] - 2
    before = lax.slice_in_dim(widened, 0, length, axis=axis_pos)
    middle = lax.slice_in_dim(widened, 1, length + 1, axis=axis_pos)
    beyond = lax.slice_in_dim(widened, 2, length + 2, axis=axis_pos)
    even_rows = 0.25 * before + 0.75 * middle
    odd_rows = 0.75 * middle + 0.25 * beyond
    stacked = jnp.stack([even_rows, odd_rows], axis_pos + 1)
    new_shape = list(widened.shape)
    new_shape[axis_pos] = 2 * length
    return stacked.reshape(new_shape)

def edge_columns(values):
    return jnp.concatenate([values[:, :, :1], values, values[:, :, -1:]], 2)

def lateral(feature, weight, bias_row):
    flattened = feature.reshape(-1, feature.shape[-1])
    result = jnp.dot(flattened, weight, preferred_element_type=jnp.float32) + bias_row
    return result.reshape(feature.shape[:-1] + (weight.shape[1],))

def conv_three(widened, weight):
    padded = jnp.pad(widened, ((0, 0), (0, 0), (1, 1), (0, 0)))
    strip_rows = widened.shape[1] - 2
    width_cells = widened.shape[2]
    channels = widened.shape[3]
    result = jnp.zeros((widened.shape[0] * strip_rows * width_cells, weight.shape[2]), jnp.float32)
    for tap_row in range(3):
        band_rows = padded[:, tap_row:tap_row + strip_rows]
        stacked = jnp.concatenate([band_rows[:, :, 0:width_cells], band_rows[:, :, 1:width_cells + 1], band_rows[:, :, 2:width_cells + 2]], 3)
        result = result + jnp.dot(stacked.reshape(-1, 3 * channels), weight[tap_row], preferred_element_type=jnp.float32)
    return result.reshape(widened.shape[0], strip_rows, width_cells, weight.shape[2])

def group_sums(conv_out):
    dims_all = conv_out.shape
    grouped = conv_out.reshape(dims_all[0], -1, GROUPS, dims_all[3] // GROUPS)
    return (lax.optimization_barrier(jnp.sum(grouped, axis=(1, 3))), lax.optimization_barrier(jnp.sum(grouped * grouped, axis=(1, 3))))

def normalize(conv_out, totals, squares, entries, gain_row, shift_row):
    mean_val = totals / entries
    variance = squares / entries - mean_val * mean_val
    scale_inv = lax.rsqrt(variance + epsilon)
    dims_all = conv_out.shape
    grouped = conv_out.reshape(dims_all[0], dims_all[1], dims_all[2], GROUPS, dims_all[3] // GROUPS)
    centred = (grouped - mean_val[:, None, None, :, None]) * scale_inv[:, None, None, :, None]
    return (centred.reshape(dims_all) * gain_row + shift_row).astype(jnp.bfloat16)

def reference(level_two, level_three, level_four, level_five, lateral_two, lateral_three, lateral_four, lateral_five, lateral_bias, smooth_weight, norm_gain, norm_shift):
    features = (level_two, level_three, level_four, level_five)
    weights = (lateral_two, lateral_three, lateral_four, lateral_five)
    laterals = [lateral(features[level_idx], weights[level_idx], lateral_bias[level_idx]) for level_idx in range(4)]
    merged_maps = [None, None, None, None]
    merged_maps[3] = laterals[3].astype(jnp.bfloat16)
    for level_idx in (2, 1, 0):
        coarse = merged_maps[level_idx + 1].astype(jnp.float32)
        widened = jnp.concatenate([coarse[:, :1], coarse, coarse[:, -1:]], 1)
        upsampled = refine(edge_columns(refine(widened, 1)), 2)
        merged_maps[level_idx] = (laterals[level_idx] + upsampled).astype(jnp.bfloat16)
    outputs = []
    for level_idx in range(4):
        widened = jnp.pad(merged_maps[level_idx], ((0, 0), (1, 1), (0, 0), (0, 0)))
        conv_out = conv_three(widened, smooth_weight[level_idx])
        totals, squares = group_sums(conv_out)
        entries = float(conv_out.shape[1] * conv_out.shape[2] * (conv_out.shape[3] // GROUPS))
        outputs.append(normalize(conv_out, totals, squares, entries, norm_gain[level_idx], norm_shift[level_idx]))
    return (outputs[0], outputs[1], outputs[2], outputs[3])
```

```python
import functools

import jax
import jax.numpy as jnp
from jax import lax
from jax.experimental import pallas as pl
from jax.experimental.pallas import tpu as pltpu
from jax.sharding import PartitionSpec as P

GROUPS = 32
EPSILON = 1e-05
F32 = jnp.float32
BF16 = jnp.bfloat16
MIB = 1 << 20


def dot(a, b):
    return jnp.dot(a, b, preferred_element_type=F32)


def flat(v):
    return v.reshape(-1, v.shape[-1])


def segments(widths):
    offsets, total = [], 0
    for width in widths:
        offsets.append(total)
        total += width
    return offsets, total


def lateral_kernel(
    x2, x3, x4, x5, w2, w3, w4, w5, bias,
    lat3, lat4, lat5, downward, upward,
    edge2, v3, v4, v5, m2, m3, m4, m5, sems,
):
    rows2 = x2.shape[1]
    moves = [
        (x5, v5), (w5, m5), (x4, v4), (w4, m4), (x3, v3), (w3, m3),
        (x2.at[:, 0], edge2.at[0]), (x2.at[:, rows2 - 1], edge2.at[1]), (w2, m2),
    ]
    copies = [
        pltpu.make_async_copy(src, dst, sems.at[n]) for n, (src, dst) in enumerate(moves)
    ]
    for c in copies:
        c.start()
    widths = (x2.shape[2], x3.shape[2], x4.shape[2], x5.shape[2])
    offsets, _ = segments(widths)
    images = x2.shape[0]
    first = 0
    for level, v, m, out in ((3, v5, m5, lat5), (2, v4, m4, lat4), (1, v3, m3, lat3)):
        copies[first].wait()
        copies[first + 1].wait()
        first += 2
        res = dot(flat(v[...]), m[...]) + bias[level : level + 1, :]
        res = res.reshape(out.shape)
        out[...] = res
        seg = slice(offsets[level], offsets[level] + widths[level])
        downward[:, seg, :] = res[:, out.shape[1] - 1].astype(BF16)
        upward[:, seg, :] = res[:, 0].astype(BF16)
    for n in (6, 7, 8):
        copies[n].wait()
    for side, ref in ((0, upward), (1, downward)):
        res = dot(flat(edge2[side]), m2[...]) + bias[0:1, :]
        ref[:, 0 : widths[0], :] = res.reshape(images, widths[0], -1).astype(BF16)


def fill_weights(table):
    _, fine, twice = table.shape
    coarse = twice // 2
    row = lax.broadcasted_iota(jnp.int32, (fine, twice), 0)
    col = lax.broadcasted_iota(jnp.int32, (fine, twice), 1)
    second = col >= coarse
    col = jnp.where(second, col - coarse, col)
    near = row // 2
    far = jnp.clip(jnp.where(row % 2 == 0, near - 1, near + 1), 0, coarse - 1)
    base = jnp.where(col == near, 0.75, 0.0) + jnp.where(col == far, 0.25, 0.0)
    for n, (a, b) in enumerate(((0.25, 0.75), (0.75, 0.25), (0.0, 1.0), (1.0, 0.0))):
        table[n] = (base * jnp.where(second, b, a)).astype(BF16)


def conv_kernel(
    ends, x2, w2, bias, lat3, lat4, lat5, above, below, smooth,
    conv2, conv3, conv4, conv5, stats,
    v2, m2, sw, cat2, cat3, cat4, cat5, u2, u3, u4, sems,
):
    copies = [pltpu.make_async_copy(w2, m2, sems.at[0])]
    images, rows2, cols2, _ = x2.shape
    for i in range(images):
        copies.append(pltpu.make_async_copy(x2.at[i], v2.at[i], sems.at[1 + i]))
    for level in range(4):
        copies.append(
            pltpu.make_async_copy(smooth.at[level], sw.at[level], sems.at[1 + images + level])
        )
    for c in copies:
        c.start()
    is_first = ends[0] == 1
    is_last = ends[1] == 1
    cats = (cat2, cat3, cat4, cat5)
    tables = (u2, u3, u4)
    lats = (None, lat3, lat4, lat5)
    channels = lat3.shape[-1]
    for table in tables:
        fill_weights(table)
    widths = tuple(cat.shape[2] for cat in cats)
    heights = tuple(cat.shape[1] - 2 for cat in cats)
    offsets, _ = segments(widths)

    def put(level, image, slot, acc):
        cols = acc.shape[0]
        cat = cats[level]
        row = lax.broadcasted_iota(jnp.int32, acc.shape, 0)
        left = jnp.where(row == 0, 0.0, pltpu.roll(acc, 1, 0))
        right = jnp.where(row == cols - 1, 0.0, pltpu.roll(acc, cols - 1, 0))
        cat[image, slot, :, 0:channels] = left.astype(BF16)
        cat[image, slot, :, channels : 2 * channels] = acc.astype(BF16)
        cat[image, slot, :, 2 * channels : 3 * channels] = right.astype(BF16)

    def raised(level, image, start, which):
        below_cat = cats[level + 1]
        pair = below_cat[image, pl.ds(start, 2), :, channels : 2 * channels]
        return dot(tables[level][which], flat(pair))

    def halos(level, image):
        seg = slice(offsets[level], offsets[level] + widths[level])
        height = heights[level]
        for slot, source, gone, which in (
            (0, above, is_first, 1),
            (height + 1, below, is_last, 0),
        ):
            acc = source[image, seg, :].astype(F32)
            if level < 3:
                acc = acc + raised(level, image, slot // 2, which)
            put(level, image, slot, jnp.where(gone, 0.0, acc))

    for level in (3, 2, 1):
        height = heights[level]
        for image in range(images):
            halos(level, image)
            for f in range(height):
                acc = lats[level][image, f]
                if level < 3:
                    which = f % 2
                    if f == 0:
                        which = jnp.where(is_first, 2, which)
                    if f == height - 1:
                        which = jnp.where(is_last, 3, which)
                    acc = acc + raised(level, image, (f + 1) // 2, which)
                put(level, image, f + 1, acc)
    copies[0].wait()
    for image in range(images):
        halos(0, image)
        copies[1 + image].wait()

        def pair_rows(j, carry, image=image):
            for odd in range(2):
                f = 2 * j + odd
                if odd:
                    which = jnp.where(jnp.logical_and(is_last, f == rows2 - 1), 3, 1)
                else:
                    which = jnp.where(jnp.logical_and(is_first, f == 0), 2, 0)
                acc = dot(v2[image, f], m2[...]) + bias[0:1, :]
                acc = acc + raised(0, image, j + odd, which)
                put(0, image, f + 1, acc)
            return carry

        lax.fori_loop(0, rows2 // 2, pair_rows, 0)

    def sums(res):
        part = res.reshape(-1, 8, channels)
        return jnp.sum(part, axis=0), jnp.sum(part * part, axis=0)

    def taps(level, lhs_of):
        acc = dot(lhs_of(0), sw[level, 0])
        acc = acc + dot(lhs_of(1), sw[level, 1])
        return acc + dot(lhs_of(2), sw[level, 2])

    step = 4 if rows2 % 4 == 0 else 2
    copies[1 + images].wait()
    for image in range(images):

        def strip(n, carry, image=image):
            r = n * step
            acc = taps(0, lambda a: flat(cat2[image, pl.ds(r + a, step)]))
            conv2[image, pl.ds(r, step)] = acc.reshape(step, cols2, channels)
            s, q = sums(acc)
            return carry[0] + s, carry[1] + q

        zero = jnp.zeros((8, channels), F32)
        s, q = lax.fori_loop(0, rows2 // step, strip, (zero, zero))
        stats[2 * image : 2 * image + 1, :] = jnp.sum(s, axis=0, keepdims=True)
        stats[2 * image + 1 : 2 * image + 2, :] = jnp.sum(q, axis=0, keepdims=True)
    for level, out in ((1, conv3), (2, conv4), (3, conv5)):
        copies[1 + images + level].wait()
        height = heights[level]
        acc = taps(level, lambda a: flat(cats[level][:, a : a + height]))
        acc = acc.reshape(images, -1, channels)
        out[...] = acc.reshape(out.shape)
        for image in range(images):
            s, q = sums(acc[image])
            at = 2 * (images * level + image)
            stats[at : at + 1, :] = jnp.sum(s, axis=0, keepdims=True)
            stats[at + 1 : at + 2, :] = jnp.sum(q, axis=0, keepdims=True)


def norm_kernel(
    conv2, conv3, conv4, conv5, totals, gain, shift,
    out2, out3, out4, out5,
    s2, s3, s4, s5, sems, *, strips,
):
    channels = conv2.shape[-1]
    width = channels // GROUPS
    row = lax.broadcasted_iota(jnp.int32, (channels, channels), 0) // width
    col = lax.broadcasted_iota(jnp.int32, (channels, channels), 1) // width
    same = jnp.where(row == col, 1.0, 0.0).astype(F32)
    grouped = jnp.dot(
        totals[...], same, precision=lax.Precision.HIGHEST, preferred_element_type=F32
    )
    images = conv2.shape[0]
    copies = []
    levels = ((conv2, s2, out2), (conv3, s3, out3), (conv4, s4, out4), (conv5, s5, out5))
    for level, (conv, stage, out) in enumerate(levels):
        entries = float(conv.shape[1] * strips * conv.shape[2] * width)
        for image in range(images):
            at = 2 * (images * level + image)
            mean = grouped[at : at + 1, :] / entries
            variance = grouped[at + 1 : at + 2, :] / entries - mean * mean
            scale = lax.rsqrt(variance + EPSILON) * gain[level : level + 1, :]
            offset = shift[level : level + 1, :]
            height = conv.shape[1]
            block = min(height, 4)
            for r in range(0, height, block):
                part = flat(conv[image, r : r + block])
                done = ((part - mean) * scale + offset).astype(BF16)
                stage[image, r : r + block] = done.reshape(block, conv.shape[2], channels)
                copy = pltpu.make_async_copy(
                    stage.at[image, pl.ds(r, block)],
                    out.at[image, pl.ds(r, block)],
                    sems.at[len(copies)],
                )
                copy.start()
                copies.append(copy)
    for copy in copies:
        copy.wait()


def total_over(x, axis):
    count = lax.axis_size(axis)
    if count & (count - 1):
        return lax.psum(x, axis)
    step = 1
    while step < count:
        x = x + lax.ppermute(x, axis, [(i, i ^ step) for i in range(count)])
        step *= 2
    return x


def per_device(
    level_two, level_three, level_four, level_five,
    lateral_two, lateral_three, lateral_four, lateral_five,
    lateral_bias, smooth_weight, norm_gain, norm_shift,
):
    position = lax.axis_index("rows")
    strips = lax.axis_size("rows")
    levels = (level_two, level_three, level_four, level_five)
    laterals = (lateral_two, lateral_three, lateral_four, lateral_five)
    images = level_two.shape[0]
    channels = lateral_two.shape[1]
    widths = tuple(v.shape[2] for v in levels)
    heights = tuple(v.shape[1] for v in levels)
    _, pack = segments(widths)
    hbm = pl.BlockSpec(memory_space=pltpu.HBM)
    vmem = pl.BlockSpec(memory_space=pltpu.VMEM)
    smem = pl.BlockSpec(memory_space=pltpu.SMEM)
    like = lambda v: pltpu.VMEM(v.shape, v.dtype)
    maps = [
        jax.ShapeDtypeStruct((images, heights[k], widths[k], channels), F32) for k in range(4)
    ]
    packed = jax.ShapeDtypeStruct((images, pack, channels), BF16)
    lat3, lat4, lat5, downward, upward = pl.pallas_call(
        lateral_kernel,
        out_shape=(maps[1], maps[2], maps[3], packed, packed),
        in_specs=[hbm] * 8 + [vmem],
        out_specs=[vmem] * 5,
        scratch_shapes=[
            pltpu.VMEM((2, images) + level_two.shape[2:], level_two.dtype),
            like(level_three), like(level_four), like(level_five),
            like(lateral_two), like(lateral_three), like(lateral_four), like(lateral_five),
            pltpu.SemaphoreType.DMA((9,)),
        ],
        compiler_params=pltpu.CompilerParams(vmem_limit_bytes=20 * MIB),
        name="laterals",
    )(*levels, *laterals, lateral_bias)
    ends = strips - 1
    above = lax.ppermute(downward, "rows", [(i, i + 1) for i in range(ends)])
    below = lax.ppermute(upward, "rows", [(i + 1, i) for i in range(ends)])
    flags = jnp.stack([position == 0, position == ends]).astype(jnp.int32)
    cat = lambda k: pltpu.VMEM((images, heights[k] + 2, widths[k], 3 * channels), BF16)
    table = lambda k: pltpu.VMEM((4, widths[k], 2 * widths[k + 1]), BF16)
    convs = pl.pallas_call(
        conv_kernel,
        out_shape=tuple(maps) + (jax.ShapeDtypeStruct((8 * images, channels), F32),),
        in_specs=[smem, hbm, hbm] + [vmem] * 6 + [hbm],
        out_specs=[vmem] * 5,
        scratch_shapes=[
            like(level_two), like(lateral_two), like(smooth_weight),
            cat(0), cat(1), cat(2), cat(3), table(0), table(1), table(2),
            pltpu.SemaphoreType.DMA((5 + images,)),
        ],
        compiler_params=pltpu.CompilerParams(vmem_limit_bytes=40 * MIB),
        name="merge_conv",
    )(
        flags, level_two, lateral_two, lateral_bias, lat3, lat4, lat5, above, below,
        smooth_weight,
    )
    totals = total_over(convs[4], "rows")
    outs = [jax.ShapeDtypeStruct(m.shape, BF16) for m in maps]
    count = images * sum(h // min(h, 4) for h in heights)
    return tuple(
        pl.pallas_call(
            functools.partial(norm_kernel, strips=strips),
            out_shape=tuple(outs),
            in_specs=[vmem] * 7,
            out_specs=[hbm] * 4,
            scratch_shapes=[like(o) for o in outs] + [pltpu.SemaphoreType.DMA((count,))],
            compiler_params=pltpu.CompilerParams(vmem_limit_bytes=20 * MIB),
            name="normalize",
        )(*convs[:4], totals, norm_gain, norm_shift)
    )


def solution(mesh):
    split = P("batch", "rows", None, None)
    return jax.shard_map(
        per_device,
        mesh=mesh,
        in_specs=(split,) * 4 + (P(),) * 8,
        out_specs=(split,) * 4,
        check_vma=False,
    )
```

```python
import functools

import jax
import jax.numpy as jnp
from jax import lax
from jax.experimental import pallas as pl
from jax.experimental.pallas import tpu as pltpu
from jax.sharding import PartitionSpec as P

GROUPS = 32
EPSILON = 1e-05
F32 = jnp.float32
BF16 = jnp.bfloat16
MIB = 1 << 20


def dot(a, b):
    return jnp.dot(a, b, preferred_element_type=F32)


def flat(v):
    return v.reshape(-1, v.shape[-1])


def segments(widths):
    offsets, total = [], 0
    for width in widths:
        offsets.append(total)
        total += width
    return offsets, total


def lateral_kernel(
    x2, x3, x4, x5, w2, w3, w4, w5, bias,
    lat3, lat4, lat5, downward, upward, downward2, upward2,
    edge2, v3, v4, v5, m2, m3, m4, m5, sems,
):
    rows2 = x2.shape[1]
    moves = [
        (x5, v5), (w5, m5), (x4, v4), (w4, m4), (x3, v3), (w3, m3),
        (x2.at[:, 0], edge2.at[0]), (x2.at[:, rows2 - 1], edge2.at[1]), (w2, m2),
    ]
    copies = [
        pltpu.make_async_copy(src, dst, sems.at[n]) for n, (src, dst) in enumerate(moves)
    ]
    for c in copies:
        c.start()
    widths = (x3.shape[2], x4.shape[2], x5.shape[2])
    offsets, _ = segments(widths)
    images = x2.shape[0]
    first = 0
    for level, v, m, out in ((3, v5, m5, lat5), (2, v4, m4, lat4), (1, v3, m3, lat3)):
        copies[first].wait()
        copies[first + 1].wait()
        first += 2
        res = dot(flat(v[...]), m[...]) + bias[level : level + 1, :]
        res = res.reshape(out.shape)
        out[...] = res
        seg = slice(offsets[level - 1], offsets[level - 1] + widths[level - 1])
        downward[:, seg, :] = res[:, out.shape[1] - 1].astype(BF16)
        upward[:, seg, :] = res[:, 0].astype(BF16)
    for n in (6, 7, 8):
        copies[n].wait()
    for side, ref in ((0, upward2), (1, downward2)):
        res = dot(flat(edge2[side]), m2[...]) + bias[0:1, :]
        ref[...] = res.reshape(ref.shape).astype(BF16)


def fill_weights(table):
    _, fine, twice = table.shape
    coarse = twice // 2
    row = lax.broadcasted_iota(jnp.int32, (fine, twice), 0)
    col = lax.broadcasted_iota(jnp.int32, (fine, twice), 1)
    second = col >= coarse
    col = jnp.where(second, col - coarse, col)
    near = row // 2
    far = jnp.clip(jnp.where(row % 2 == 0, near - 1, near + 1), 0, coarse - 1)
    base = jnp.where(col == near, 0.75, 0.0) + jnp.where(col == far, 0.25, 0.0)
    for n, (a, b) in enumerate(((0.25, 0.75), (0.75, 0.25), (0.0, 1.0), (1.0, 0.0))):
        table[n] = (base * jnp.where(second, b, a)).astype(BF16)


def put(cat, image, slot, acc):
    cols, channels = acc.shape
    row = lax.broadcasted_iota(jnp.int32, acc.shape, 0)
    left = jnp.where(row == 0, 0.0, pltpu.roll(acc, 1, 0))
    right = jnp.where(row == cols - 1, 0.0, pltpu.roll(acc, cols - 1, 0))
    cat[image, slot, :, 0:channels] = left.astype(BF16)
    cat[image, slot, :, channels : 2 * channels] = acc.astype(BF16)
    cat[image, slot, :, 2 * channels : 3 * channels] = right.astype(BF16)


def note_sums(stats, at, res):
    part = res.reshape(-1, 8, res.shape[-1])
    stats[at : at + 1, :] = jnp.sum(jnp.sum(part, axis=0), axis=0, keepdims=True)
    stats[at + 1 : at + 2, :] = jnp.sum(jnp.sum(part * part, axis=0), axis=0, keepdims=True)


def coarse_kernel(
    ends, x2, w2, bias, lat3, lat4, lat5, above, below, smooth,
    conv3, conv4, conv5, stats, cat2, rim2, sw2,
    v2, m2, sw, cat3, cat4, cat5, u2, u3, u4, sems,
):
    copies = [pltpu.make_async_copy(w2, m2, sems.at[0])]
    images, rows2, cols2, _ = x2.shape
    for i in range(images):
        copies.append(pltpu.make_async_copy(x2.at[i], v2.at[i], sems.at[1 + i]))
    for level in (1, 2, 3, 0):
        copies.append(
            pltpu.make_async_copy(
                smooth.at[level],
                sw.at[level - 1] if level else sw2,
                sems.at[1 + images + level],
            )
        )
    for c in copies:
        c.start()
    is_first = ends[0] == 1
    is_last = ends[1] == 1
    cats = (cat2, cat3, cat4, cat5)
    tables = (u2, u3, u4)
    lats = (None, lat3, lat4, lat5)
    channels = lat3.shape[-1]
    for table in tables:
        fill_weights(table)
    offsets, _ = segments(tuple(cat.shape[2] for cat in cats[1:]))

    def raised(level, image, start, which):
        pair = cats[level + 1][image, pl.ds(start, 2), :, channels : 2 * channels]
        return dot(tables[level][which], flat(pair))

    for level in (3, 2, 1):
        height, cols = lats[level].shape[1:3]
        seg = slice(offsets[level - 1], offsets[level - 1] + cols)
        for image in range(images):
            for slot, source, gone, which in (
                (0, above, is_first, 1),
                (height + 1, below, is_last, 0),
            ):
                acc = source[image, seg, :].astype(F32)
                if level < 3:
                    acc = acc + raised(level, image, slot // 2, which)
                put(cats[level], image, slot, jnp.where(gone, 0.0, acc))
            for f in range(height):
                acc = lats[level][image, f]
                if level < 3:
                    which = f % 2
                    if f == 0:
                        which = jnp.where(is_first, 2, which)
                    if f == height - 1:
                        which = jnp.where(is_last, 3, which)
                    acc = acc + raised(level, image, (f + 1) // 2, which)
                put(cats[level], image, f + 1, acc)
    copies[0].wait()
    for image in range(images):
        rim2[0, image] = raised(0, image, 0, 1)
        rim2[1, image] = raised(0, image, rows2 // 2, 0)
        copies[1 + image].wait()

        def pair_rows(j, carry, image=image):
            for odd in range(2):
                f = 2 * j + odd
                if odd:
                    which = jnp.where(jnp.logical_and(is_last, f == rows2 - 1), 3, 1)
                else:
                    which = jnp.where(jnp.logical_and(is_first, f == 0), 2, 0)
                acc = dot(v2[image, f], m2[...]) + bias[0:1, :]
                acc = acc + raised(0, image, j + odd, which)
                put(cat2, image, f, acc)
            return carry

        lax.fori_loop(0, rows2 // 2, pair_rows, 0)

    for level, out in ((1, conv3), (2, conv4), (3, conv5)):
        copies[images + level].wait()
        height = out.shape[1]
        lhs = lambda a: flat(cats[level][:, a : a + height])
        acc = dot(lhs(0), sw[level - 1, 0])
        acc = acc + dot(lhs(1), sw[level - 1, 1])
        acc = acc + dot(lhs(2), sw[level - 1, 2])
        acc = acc.reshape(images, -1, channels)
        out[...] = acc.reshape(out.shape)
        for image in range(images):
            note_sums(stats, 2 * (images * (level - 1) + image), acc[image])
    copies[images + 4].wait()


def fine_kernel(ends, cat2, rim2, sw2, above2, below2, coarse_stats, conv2, stats, halo):
    images, rows2, cols2, _ = cat2.shape
    channels = conv2.shape[-1]
    step = 4 if rows2 % 4 == 0 else 2
    stats[2 * images :, :] = coarse_stats[...]
    for image in range(images):
        for side, source in ((0, above2), (1, below2)):
            acc = source[image].astype(F32) + rim2[side, image]
            put(halo, side, image, jnp.where(ends[side] == 1, 0.0, acc))
    for image in range(images):
        total = square = jnp.zeros((8, channels), F32)
        for r in range(0, rows2, step):
            acc = None
            for tap in range(3):
                low, high = r + tap - 1, r + tap - 1 + step
                lhs = cat2[image, max(low, 0) : min(high, rows2)]
                if low < 0:
                    lhs = jnp.concatenate([halo[0, image][None], lhs], 0)
                if high > rows2:
                    lhs = jnp.concatenate([lhs, halo[1, image][None]], 0)
                res = dot(flat(lhs), sw2[tap])
                acc = res if acc is None else acc + res
            conv2[image, r : r + step] = acc.reshape(step, cols2, channels)
            part = acc.reshape(-1, 8, channels)
            total = total + jnp.sum(part, axis=0)
            square = square + jnp.sum(part * part, axis=0)
        stats[2 * image : 2 * image + 1, :] = jnp.sum(total, axis=0, keepdims=True)
        stats[2 * image + 1 : 2 * image + 2, :] = jnp.sum(square, axis=0, keepdims=True)


def norm_kernel(
    conv2, conv3, conv4, conv5, totals, gain, shift,
    out2, out3, out4, out5,
    s2, s3, s4, s5, sems, *, strips,
):
    channels = conv2.shape[-1]
    width = channels // GROUPS
    row = lax.broadcasted_iota(jnp.int32, (channels, channels), 0) // width
    col = lax.broadcasted_iota(jnp.int32, (channels, channels), 1) // width
    same = jnp.where(row == col, 1.0, 0.0).astype(F32)
    grouped = jnp.dot(
        totals[...], same, precision=lax.Precision.HIGHEST, preferred_element_type=F32
    )
    images = conv2.shape[0]
    copies = []
    levels = ((conv2, s2, out2), (conv3, s3, out3), (conv4, s4, out4), (conv5, s5, out5))
    for level, (conv, stage, out) in enumerate(levels):
        entries = float(conv.shape[1] * strips * conv.shape[2] * width)
        for image in range(images):
            at = 2 * (images * level + image)
            mean = grouped[at : at + 1, :] / entries
            variance = grouped[at + 1 : at + 2, :] / entries - mean * mean
            scale = lax.rsqrt(variance + EPSILON) * gain[level : level + 1, :]
            offset = shift[level : level + 1, :]
            height = conv.shape[1]
            block = min(height, 4)
            for r in range(0, height, block):
                part = flat(conv[image, r : r + block])
                done = ((part - mean) * scale + offset).astype(BF16)
                stage[image, r : r + block] = done.reshape(block, conv.shape[2], channels)
                copy = pltpu.make_async_copy(
                    stage.at[image, pl.ds(r, block)],
                    out.at[image, pl.ds(r, block)],
                    sems.at[len(copies)],
                )
                copy.start()
                copies.append(copy)
    for copy in copies:
        copy.wait()


def total_over(x, axis):
    count = lax.axis_size(axis)
    if count & (count - 1):
        return lax.psum(x, axis)
    step = 1
    while step < count:
        x = x + lax.ppermute(x, axis, [(i, i ^ step) for i in range(count)])
        step *= 2
    return x


def per_device(
    level_two, level_three, level_four, level_five,
    lateral_two, lateral_three, lateral_four, lateral_five,
    lateral_bias, smooth_weight, norm_gain, norm_shift,
):
    position = lax.axis_index("rows")
    strips = lax.axis_size("rows")
    levels = (level_two, level_three, level_four, level_five)
    laterals = (lateral_two, lateral_three, lateral_four, lateral_five)
    levels = tuple(pltpu.with_memory_space_constraint(v, pltpu.HBM) for v in levels)
    laterals = tuple(pltpu.with_memory_space_constraint(v, pltpu.HBM) for v in laterals)
    smooth = pltpu.with_memory_space_constraint(smooth_weight, pltpu.HBM)
    images = level_two.shape[0]
    channels = lateral_two.shape[1]
    widths = tuple(v.shape[2] for v in levels)
    heights = tuple(v.shape[1] for v in levels)
    _, pack = segments(widths[1:])
    hbm = pl.BlockSpec(memory_space=pltpu.HBM)
    vmem = pl.BlockSpec(memory_space=pltpu.VMEM)
    smem = pl.BlockSpec(memory_space=pltpu.SMEM)
    like = lambda v: pltpu.VMEM(v.shape, v.dtype)
    shape = jax.ShapeDtypeStruct
    maps = [shape((images, heights[k], widths[k], channels), F32) for k in range(4)]
    packed = shape((images, pack, channels), BF16)
    packed2 = shape((images, widths[0], channels), BF16)
    lat3, lat4, lat5, downward, upward, downward2, upward2 = pl.pallas_call(
        lateral_kernel,
        out_shape=(maps[1], maps[2], maps[3], packed, packed, packed2, packed2),
        in_specs=[hbm] * 8 + [vmem],
        out_specs=[vmem] * 7,
        scratch_shapes=[
            pltpu.VMEM((2, images) + level_two.shape[2:], level_two.dtype),
            like(level_three), like(level_four), like(level_five),
            like(lateral_two), like(lateral_three), like(lateral_four), like(lateral_five),
            pltpu.SemaphoreType.DMA((9,)),
        ],
        compiler_params=pltpu.CompilerParams(vmem_limit_bytes=20 * MIB),
        name="laterals",
    )(*levels, *laterals, lateral_bias)
    ends = strips - 1
    from_above = lambda v: lax.ppermute(v, "rows", [(i, i + 1) for i in range(ends)])
    from_below = lambda v: lax.ppermute(v, "rows", [(i + 1, i) for i in range(ends)])
    above, below = from_above(downward), from_below(upward)
    above2, below2 = from_above(downward2), from_below(upward2)
    flags = jnp.stack([position == 0, position == ends]).astype(jnp.int32)
    cat = lambda k: pltpu.VMEM((images, heights[k] + 2, widths[k], 3 * channels), BF16)
    table = lambda k: pltpu.VMEM((4, widths[k], 2 * widths[k + 1]), BF16)
    conv3, conv4, conv5, coarse_stats, cat2, rim2, sw2 = pl.pallas_call(
        coarse_kernel,
        out_shape=(
            maps[1], maps[2], maps[3], shape((6 * images, channels), F32),
            shape((images, heights[0], widths[0], 3 * channels), BF16),
            shape((2, images, widths[0], channels), F32),
            shape(smooth_weight.shape[1:], BF16),
        ),
        in_specs=[smem, hbm, hbm] + [vmem] * 6 + [hbm],
        out_specs=[vmem] * 7,
        scratch_shapes=[
            like(level_two), like(lateral_two),
            pltpu.VMEM((3,) + smooth_weight.shape[1:], BF16),
            cat(1), cat(2), cat(3), table(0), table(1), table(2),
            pltpu.SemaphoreType.DMA((5 + images,)),
        ],
        compiler_params=pltpu.CompilerParams(vmem_limit_bytes=24 * MIB),
        name="merge_coarse",
    )(flags, levels[0], laterals[0], lateral_bias, lat3, lat4, lat5, above, below, smooth)
    conv2, stats = pl.pallas_call(
        fine_kernel,
        out_shape=(maps[0], shape((8 * images, channels), F32)),
        in_specs=[smem] + [vmem] * 6,
        out_specs=[vmem] * 2,
        scratch_shapes=[pltpu.VMEM((2, images, widths[0], 3 * channels), BF16)],
        compiler_params=pltpu.CompilerParams(vmem_limit_bytes=24 * MIB),
        name="conv_fine",
    )(flags, cat2, rim2, sw2, above2, below2, coarse_stats)
    convs = (conv2, conv3, conv4, conv5)
    totals = total_over(stats, "rows")
    outs = [jax.ShapeDtypeStruct(m.shape, BF16) for m in maps]
    count = images * sum(h // min(h, 4) for h in heights)
    return tuple(
        pl.pallas_call(
            functools.partial(norm_kernel, strips=strips),
            out_shape=tuple(outs),
            in_specs=[vmem] * 7,
            out_specs=[hbm] * 4,
            scratch_shapes=[like(o) for o in outs] + [pltpu.SemaphoreType.DMA((count,))],
            compiler_params=pltpu.CompilerParams(vmem_limit_bytes=20 * MIB),
            name="normalize",
        )(*convs, totals, norm_gain, norm_shift)
    )


def solution(mesh):
    split = P("batch", "rows", None, None)
    return jax.shard_map(
        per_device,
        mesh=mesh,
        in_specs=(split,) * 4 + (P(),) * 8,
        out_specs=(split,) * 4,
        check_vma=False,
    )
```

```python
import functools

import jax
import jax.numpy as jnp
from jax import lax
from jax.experimental import pallas as pl
from jax.experimental.pallas import tpu as pltpu
from jax.sharding import PartitionSpec as P


GROUPS = 32
EPSILON = 1e-05
F32 = jnp.float32
BF16 = jnp.bfloat16
MIB = 1 << 20


def dot(a, b):
    return jnp.dot(a, b, preferred_element_type=F32)


def flat(v):
    return v.reshape(-1, v.shape[-1])


def segments(widths):
    offsets, total = [], 0
    for width in widths:
        offsets.append(total)
        total += width
    return offsets, total


def lateral_kernel(
    x2, x3, x4, x5, w2, w3, w4, w5, bias,
    lat3, lat4, lat5, downward, upward, downward2, upward2,
    edge2, v3, v4, v5, m2, m3, m4, m5, offset, sems,
):
    rows2 = x2.shape[1]
    moves = [
        (x5, v5), (w5, m5), (x4, v4), (w4, m4), (x3, v3), (w3, m3),
        (x2.at[:, 0], edge2.at[0]), (x2.at[:, rows2 - 1], edge2.at[1]), (w2, m2),
        (bias, offset),
    ]
    copies = [
        pltpu.make_async_copy(src, dst, sems.at[n]) for n, (src, dst) in enumerate(moves)
    ]
    for c in copies:
        c.start()
    widths = (x3.shape[2], x4.shape[2], x5.shape[2])
    offsets, _ = segments(widths)
    copies[9].wait()
    first = 0
    for level, v, m, out in ((3, v5, m5, lat5), (2, v4, m4, lat4), (1, v3, m3, lat3)):
        copies[first].wait()
        copies[first + 1].wait()
        first += 2
        res = dot(flat(v[...]), m[...]) + offset[level : level + 1, :]
        res = res.reshape(out.shape)
        out[...] = res
        seg = slice(offsets[level - 1], offsets[level - 1] + widths[level - 1])
        downward[:, seg, :] = res[:, out.shape[1] - 1].astype(BF16)
        upward[:, seg, :] = res[:, 0].astype(BF16)
    for n in (6, 7, 8):
        copies[n].wait()
    for side, ref in ((0, upward2), (1, downward2)):
        res = dot(flat(edge2[side]), m2[...]) + offset[0:1, :]
        ref[...] = res.reshape(ref.shape).astype(BF16)


def fill_weights(table):
    _, fine, twice = table.shape
    coarse = twice // 2
    row = lax.broadcasted_iota(jnp.int32, (fine, twice), 0)
    col = lax.broadcasted_iota(jnp.int32, (fine, twice), 1)
    second = col >= coarse
    col = jnp.where(second, col - coarse, col)
    near = row // 2
    far = jnp.clip(jnp.where(row % 2 == 0, near - 1, near + 1), 0, coarse - 1)
    base = jnp.where(col == near, 0.75, 0.0) + jnp.where(col == far, 0.25, 0.0)
    for n, (a, b) in enumerate(((0.25, 0.75), (0.75, 0.25), (0.0, 1.0), (1.0, 0.0))):
        table[n] = (base * jnp.where(second, b, a)).astype(BF16)


def put(cat, image, slot, acc):
    cols, channels = acc.shape
    row = lax.broadcasted_iota(jnp.int32, (8, channels), 0)
    left = pltpu.roll(acc, 1, 0)
    left = jnp.concatenate([jnp.where(row == 0, 0.0, left[:8]), left[8:]], 0)
    right = pltpu.roll(acc, cols - 1, 0)
    right = jnp.concatenate([right[:-8], jnp.where(row == 7, 0.0, right[-8:])], 0)
    cat[image, slot, :, 0:channels] = left.astype(BF16)
    cat[image, slot, :, channels : 2 * channels] = acc.astype(BF16)
    cat[image, slot, :, 2 * channels : 3 * channels] = right.astype(BF16)


def note_sums(stats, at, res):
    part = res.reshape(-1, 8, res.shape[-1])
    stats[at : at + 1, :] = jnp.sum(jnp.sum(part, axis=0), axis=0, keepdims=True)
    stats[at + 1 : at + 2, :] = jnp.sum(jnp.sum(part * part, axis=0), axis=0, keepdims=True)


def coarse_kernel(
    ends, x2, w2, bias, lat3, lat4, lat5, above, below, smooth,
    conv3, conv4, conv5, stats, cat2, rim2, sw2,
    v2, m2, sw, cat3, cat4, cat5, u2, u3, u4, sems,
):
    copies = [pltpu.make_async_copy(w2, m2, sems.at[0])]
    images, rows2, _, _ = x2.shape
    for i in range(images):
        copies.append(pltpu.make_async_copy(x2.at[i], v2.at[i], sems.at[1 + i]))
    for level in (1, 2, 3, 0):
        copies.append(
            pltpu.make_async_copy(
                smooth.at[level],
                sw.at[level - 1] if level else sw2,
                sems.at[1 + images + level],
            )
        )
    for c in copies:
        c.start()
    is_first = ends[0] == 1
    is_last = ends[1] == 1
    cats = (cat2, cat3, cat4, cat5)
    tables = (u2, u3, u4)
    lats = (None, lat3, lat4, lat5)
    channels = lat3.shape[-1]
    for table in tables:
        fill_weights(table)
    offsets, _ = segments(tuple(cat.shape[2] for cat in cats[1:]))

    def raised(level, image, start, which):
        pair = cats[level + 1][image, pl.ds(start, 2), :, channels : 2 * channels]
        return dot(tables[level][which], flat(pair))

    for level in (3, 2, 1):
        height, cols = lats[level].shape[1:3]
        seg = slice(offsets[level - 1], offsets[level - 1] + cols)
        for image in range(images):
            for slot, source, gone, which in (
                (0, above, is_first, 1),
                (height + 1, below, is_last, 0),
            ):
                acc = source[image, seg, :].astype(F32)
                if level < 3:
                    acc = acc + raised(level, image, slot // 2, which)
                put(cats[level], image, slot, jnp.where(gone, 0.0, acc))
            for f in range(height):
                acc = lats[level][image, f]
                if level < 3:
                    which = f % 2
                    if f == 0:
                        which = jnp.where(is_first, 2, which)
                    if f == height - 1:
                        which = jnp.where(is_last, 3, which)
                    acc = acc + raised(level, image, (f + 1) // 2, which)
                put(cats[level], image, f + 1, acc)
    copies[0].wait()
    for image in range(images):
        rim2[0, image] = raised(0, image, 0, 1)
        rim2[1, image] = raised(0, image, rows2 // 2, 0)
        copies[1 + image].wait()

        def pair_rows(j, carry, image=image):
            for odd in range(2):
                f = 2 * j + odd
                if odd:
                    which = jnp.where(jnp.logical_and(is_last, f == rows2 - 1), 3, 1)
                else:
                    which = jnp.where(jnp.logical_and(is_first, f == 0), 2, 0)
                acc = dot(v2[image, f], m2[...]) + bias[0:1, :]
                acc = acc + raised(0, image, j + odd, which)
                put(cat2, image, f, acc)
            return carry

        lax.fori_loop(0, rows2 // 2, pair_rows, 0)

    for level, out in ((1, conv3), (2, conv4), (3, conv5)):
        copies[images + level].wait()
        height = out.shape[1]
        lhs = lambda a: flat(cats[level][:, a : a + height])
        acc = dot(lhs(0), sw[level - 1, 0])
        acc = acc + dot(lhs(1), sw[level - 1, 1])
        acc = acc + dot(lhs(2), sw[level - 1, 2])
        acc = acc.reshape(images, -1, channels)
        out[...] = acc.reshape(out.shape)
        for image in range(images):
            note_sums(stats, 2 * (images * (level - 1) + image), acc[image])
    copies[images + 4].wait()


def fine_kernel(ends, cat2, rim2, sw2, above2, below2, coarse_stats, conv2, stats, halo):
    images, rows2, cols2, _ = cat2.shape
    channels = conv2.shape[-1]
    step = 4 if rows2 % 4 == 0 else 2
    stats[2 * images :, :] = coarse_stats[...]
    for image in range(images):
        for side, source in ((0, above2), (1, below2)):
            acc = source[image].astype(F32) + rim2[side, image]
            put(halo, side, image, jnp.where(ends[side] == 1, 0.0, acc))
    for image in range(images):
        total = square = jnp.zeros((8, channels), F32)
        for r in range(0, rows2, step):
            acc = None
            for tap in range(3):
                low, high = r + tap - 1, r + tap - 1 + step
                lhs = cat2[image, max(low, 0) : min(high, rows2)]
                if low < 0:
                    lhs = jnp.concatenate([halo[0, image][None], lhs], 0)
                if high > rows2:
                    lhs = jnp.concatenate([lhs, halo[1, image][None]], 0)
                res = dot(flat(lhs), sw2[tap])
                acc = res if acc is None else acc + res
            conv2[image, r : r + step] = acc.reshape(step, cols2, channels)
            part = acc.reshape(-1, 8, channels)
            total = total + jnp.sum(part, axis=0)
            square = square + jnp.sum(part * part, axis=0)
        stats[2 * image : 2 * image + 1, :] = jnp.sum(total, axis=0, keepdims=True)
        stats[2 * image + 1 : 2 * image + 2, :] = jnp.sum(square, axis=0, keepdims=True)


def norm_kernel(
    conv2, conv3, conv4, conv5, totals, gain, shift,
    out2, out3, out4, out5,
    s2, s3, s4, s5, sems, *, strips,
):
    channels = conv2.shape[-1]
    width = channels // GROUPS
    row = lax.broadcasted_iota(jnp.int32, (channels, channels), 0) // width
    col = lax.broadcasted_iota(jnp.int32, (channels, channels), 1) // width
    same = jnp.where(row == col, 1.0, 0.0).astype(F32)
    grouped = jnp.dot(
        totals[...], same, precision=lax.Precision.HIGHEST, preferred_element_type=F32
    )
    images = conv2.shape[0]
    copies = []
    levels = ((conv2, s2, out2), (conv3, s3, out3), (conv4, s4, out4), (conv5, s5, out5))
    for level, (conv, stage, out) in enumerate(levels):
        entries = float(conv.shape[1] * strips * conv.shape[2] * width)
        for image in range(images):
            at = 2 * (images * level + image)
            mean = grouped[at : at + 1, :] / entries
            variance = grouped[at + 1 : at + 2, :] / entries - mean * mean
            scale = lax.rsqrt(variance + EPSILON) * gain[level : level + 1, :]
            offset = shift[level : level + 1, :]
            height = conv.shape[1]
            block = min(height, 4)
            for r in range(0, height, block):
                part = flat(conv[image, r : r + block])
                done = ((part - mean) * scale + offset).astype(BF16)
                stage[image, r : r + block] = done.reshape(block, conv.shape[2], channels)
                copy = pltpu.make_async_copy(
                    stage.at[image, pl.ds(r, block)],
                    out.at[image, pl.ds(r, block)],
                    sems.at[len(copies)],
                )
                copy.start()
                copies.append(copy)
    for copy in copies:
        copy.wait()


def total_over(x, axis):
    count = lax.axis_size(axis)
    if count & (count - 1):
        return lax.psum(x, axis)
    step = 1
    while step < count:
        x = x + lax.ppermute(x, axis, [(i, i ^ step) for i in range(count)])
        step *= 2
    return x


def per_device(
    level_two, level_three, level_four, level_five,
    lateral_two, lateral_three, lateral_four, lateral_five,
    lateral_bias, smooth_weight, norm_gain, norm_shift,
):
    position = lax.axis_index("rows")
    strips = lax.axis_size("rows")
    levels = (level_two, level_three, level_four, level_five)
    laterals = (lateral_two, lateral_three, lateral_four, lateral_five)
    levels = tuple(pltpu.with_memory_space_constraint(v, pltpu.HBM) for v in levels)
    laterals = tuple(pltpu.with_memory_space_constraint(v, pltpu.HBM) for v in laterals)
    smooth = pltpu.with_memory_space_constraint(smooth_weight, pltpu.HBM)
    images = level_two.shape[0]
    channels = lateral_two.shape[1]
    widths = tuple(v.shape[2] for v in levels)
    heights = tuple(v.shape[1] for v in levels)
    _, pack = segments(widths[1:])
    hbm = pl.BlockSpec(memory_space=pltpu.HBM)
    vmem = pl.BlockSpec(memory_space=pltpu.VMEM)
    smem = pl.BlockSpec(memory_space=pltpu.SMEM)
    like = lambda v: pltpu.VMEM(v.shape, v.dtype)
    shape = jax.ShapeDtypeStruct
    maps = [shape((images, heights[k], widths[k], channels), F32) for k in range(4)]
    packed = shape((images, pack, channels), BF16)
    packed2 = shape((images, widths[0], channels), BF16)
    lat3, lat4, lat5, downward, upward, downward2, upward2 = pl.pallas_call(
        lateral_kernel,
        out_shape=(maps[1], maps[2], maps[3], packed, packed, packed2, packed2),
        in_specs=[hbm] * 9,
        out_specs=[vmem] * 7,
        scratch_shapes=[
            pltpu.VMEM((2, images) + level_two.shape[2:], level_two.dtype),
            like(level_three), like(level_four), like(level_five),
            like(lateral_two), like(lateral_three), like(lateral_four), like(lateral_five),
            like(lateral_bias), pltpu.SemaphoreType.DMA((10,)),
        ],
        compiler_params=pltpu.CompilerParams(vmem_limit_bytes=20 * MIB),
        name="laterals",
    )(*levels, *laterals, pltpu.with_memory_space_constraint(lateral_bias, pltpu.HBM))
    ends = strips - 1
    from_above = lambda v: lax.ppermute(v, "rows", [(i, i + 1) for i in range(ends)])
    from_below = lambda v: lax.ppermute(v, "rows", [(i + 1, i) for i in range(ends)])
    above, below = from_above(downward), from_below(upward)
    above2, below2 = from_above(downward2), from_below(upward2)
    flags = jnp.stack([position == 0, position == ends]).astype(jnp.int32)
    cat = lambda k: pltpu.VMEM((images, heights[k] + 2, widths[k], 3 * channels), BF16)
    table = lambda k: pltpu.VMEM((4, widths[k], 2 * widths[k + 1]), BF16)
    conv3, conv4, conv5, coarse_stats, cat2, rim2, sw2 = pl.pallas_call(
        coarse_kernel,
        out_shape=(
            maps[1], maps[2], maps[3], shape((6 * images, channels), F32),
            shape((images, heights[0], widths[0], 3 * channels), BF16),
            shape((2, images, widths[0], channels), F32),
            shape(smooth_weight.shape[1:], BF16),
        ),
        in_specs=[smem, hbm, hbm] + [vmem] * 6 + [hbm],
        out_specs=[vmem] * 7,
        scratch_shapes=[
            like(level_two), like(lateral_two),
            pltpu.VMEM((3,) + smooth_weight.shape[1:], BF16),
            cat(1), cat(2), cat(3), table(0), table(1), table(2),
            pltpu.SemaphoreType.DMA((5 + images,)),
        ],
        compiler_params=pltpu.CompilerParams(vmem_limit_bytes=24 * MIB),
        name="merge_coarse",
    )(flags, levels[0], laterals[0], lateral_bias, lat3, lat4, lat5, above, below, smooth)
    conv2, stats = pl.pallas_call(
        fine_kernel,
        out_shape=(maps[0], shape((8 * images, channels), F32)),
        in_specs=[smem] + [vmem] * 6,
        out_specs=[vmem] * 2,
        scratch_shapes=[pltpu.VMEM((2, images, widths[0], 3 * channels), BF16)],
        compiler_params=pltpu.CompilerParams(vmem_limit_bytes=24 * MIB),
        name="conv_fine",
    )(flags, cat2, rim2, sw2, above2, below2, coarse_stats)
    convs = (conv2, conv3, conv4, conv5)
    totals = total_over(stats, "rows")
    outs = [jax.ShapeDtypeStruct(m.shape, BF16) for m in maps]
    count = images * sum(h // min(h, 4) for h in heights)
    return tuple(
        pl.pallas_call(
            functools.partial(norm_kernel, strips=strips),
            out_shape=tuple(outs),
            in_specs=[vmem] * 7,
            out_specs=[hbm] * 4,
            scratch_shapes=[like(o) for o in outs] + [pltpu.SemaphoreType.DMA((count,))],
            compiler_params=pltpu.CompilerParams(vmem_limit_bytes=20 * MIB),
            name="normalize",
        )(*convs, totals, norm_gain, norm_shift)
    )


def solution(mesh):
    split = P("batch", "rows", None, None)
    return jax.shard_map(
        per_device,
        mesh=mesh,
        in_specs=(split,) * 4 + (P(),) * 8,
        out_specs=(split,) * 4,
        check_vma=False,
    )
```

```python
import functools

import jax
import jax.numpy as jnp
from jax import lax
from jax.experimental import pallas as pl
from jax.experimental.pallas import tpu as pltpu
from jax.sharding import PartitionSpec as P


GROUPS = 32
EPSILON = 1e-05
F32 = jnp.float32
BF16 = jnp.bfloat16
MIB = 1 << 20


def dot(a, b):
    return jnp.dot(a, b, preferred_element_type=F32)


def flat(v):
    return v.reshape(-1, v.shape[-1])


def segments(widths):
    offsets, total = [], 0
    for width in widths:
        offsets.append(total)
        total += width
    return offsets, total


def lateral_kernel(
    x2, x3, x4, x5, w2, w3, w4, w5, bias,
    lat3, lat4, lat5, downward, upward, downward2, upward2, u2, u3, u4,
    edge2, v3, v4, v5, m2, m3, m4, m5, offset, sems,
):
    rows2 = x2.shape[1]
    moves = [
        (x5, v5), (w5, m5), (x4, v4), (w4, m4), (x3, v3), (w3, m3),
        (x2.at[:, 0], edge2.at[0]), (x2.at[:, rows2 - 1], edge2.at[1]), (w2, m2),
        (bias, offset),
    ]
    copies = [
        pltpu.make_async_copy(src, dst, sems.at[n]) for n, (src, dst) in enumerate(moves)
    ]
    for c in copies:
        c.start()
    widths = (x3.shape[2], x4.shape[2], x5.shape[2])
    offsets, _ = segments(widths)
    for table in (u4, u3, u2):
        fill_weights(table)
    copies[9].wait()
    first = 0
    for level, v, m, out in ((3, v5, m5, lat5), (2, v4, m4, lat4), (1, v3, m3, lat3)):
        copies[first].wait()
        copies[first + 1].wait()
        first += 2
        res = dot(flat(v[...]), m[...]) + offset[level : level + 1, :]
        res = res.reshape(out.shape)
        out[...] = res
        seg = slice(offsets[level - 1], offsets[level - 1] + widths[level - 1])
        downward[:, seg, :] = res[:, out.shape[1] - 1].astype(BF16)
        upward[:, seg, :] = res[:, 0].astype(BF16)
    for n in (6, 7, 8):
        copies[n].wait()
    for side, ref in ((0, upward2), (1, downward2)):
        res = dot(flat(edge2[side]), m2[...]) + offset[0:1, :]
        ref[...] = res.reshape(ref.shape).astype(BF16)


def fill_weights(table):
    _, fine, twice = table.shape
    coarse = twice // 2
    row = lax.broadcasted_iota(jnp.int32, (fine, twice), 0)
    col = lax.broadcasted_iota(jnp.int32, (fine, twice), 1)
    second = col >= coarse
    col = jnp.where(second, col - coarse, col)
    near = row // 2
    far = jnp.clip(jnp.where(row % 2 == 0, near - 1, near + 1), 0, coarse - 1)
    base = jnp.where(col == near, 0.75, 0.0) + jnp.where(col == far, 0.25, 0.0)
    for n, (a, b) in enumerate(((0.25, 0.75), (0.75, 0.25), (0.0, 1.0), (1.0, 0.0))):
        table[n] = (base * jnp.where(second, b, a)).astype(BF16)


def put(cat, image, slot, acc):
    cols, channels = acc.shape
    row = lax.broadcasted_iota(jnp.int32, (8, channels), 0)
    left = pltpu.roll(acc, 1, 0)
    left = jnp.concatenate([jnp.where(row == 0, 0.0, left[:8]), left[8:]], 0)
    right = pltpu.roll(acc, cols - 1, 0)
    right = jnp.concatenate([right[:-8], jnp.where(row == 7, 0.0, right[-8:])], 0)
    cat[image, slot, :, 0:channels] = left.astype(BF16)
    cat[image, slot, :, channels : 2 * channels] = acc.astype(BF16)
    cat[image, slot, :, 2 * channels : 3 * channels] = right.astype(BF16)


def note_sums(stats, at, res):
    part = res.reshape(-1, 8, res.shape[-1])
    stats[at : at + 1, :] = jnp.sum(jnp.sum(part, axis=0), axis=0, keepdims=True)
    stats[at + 1 : at + 2, :] = jnp.sum(jnp.sum(part * part, axis=0), axis=0, keepdims=True)


def coarse_kernel(
    ends, x2, w2, bias, lat3, lat4, lat5, u2, u3, u4, above, below, smooth,
    conv3, conv4, conv5, stats, cat2, rim2, sw2,
    v2, m2, sw, cat3, cat4, cat5, sems,
):
    copies = [pltpu.make_async_copy(w2, m2, sems.at[0])]
    images, rows2, _, _ = x2.shape
    for i in range(images):
        copies.append(pltpu.make_async_copy(x2.at[i], v2.at[i], sems.at[1 + i]))
    for level in (1, 2, 3, 0):
        copies.append(
            pltpu.make_async_copy(
                smooth.at[level],
                sw.at[level - 1] if level else sw2,
                sems.at[1 + images + level],
            )
        )
    for c in copies:
        c.start()
    is_first = ends[0] == 1
    is_last = ends[1] == 1
    cats = (cat2, cat3, cat4, cat5)
    tables = (u2, u3, u4)
    lats = (None, lat3, lat4, lat5)
    channels = lat3.shape[-1]
    offsets, _ = segments(tuple(cat.shape[2] for cat in cats[1:]))

    def raised(level, image, start, which):
        pair = cats[level + 1][image, pl.ds(start, 2), :, channels : 2 * channels]
        return dot(tables[level][which], flat(pair))

    for level in (3, 2, 1):
        height, cols = lats[level].shape[1:3]
        seg = slice(offsets[level - 1], offsets[level - 1] + cols)
        for slot, source, gone, which in (
            (0, above, is_first, 1),
            (height + 1, below, is_last, 0),
        ):
            for image in range(images):
                acc = source[image, seg, :].astype(F32)
                if level < 3:
                    acc = acc + raised(level, image, slot // 2, which)
                put(cats[level], image, slot, jnp.where(gone, 0.0, acc))
        for f in range(height):
            which = f % 2
            if f == 0:
                which = jnp.where(is_first, 2, which)
            if f == height - 1:
                which = jnp.where(is_last, 3, which)
            for image in range(images):
                acc = lats[level][image, f]
                if level < 3:
                    acc = acc + raised(level, image, (f + 1) // 2, which)
                put(cats[level], image, f + 1, acc)
    for image in range(images):
        rim2[0, image] = raised(0, image, 0, 1)
        rim2[1, image] = raised(0, image, rows2 // 2, 0)
    for n in range(1 + images):
        copies[n].wait()

    def pair_rows(j, carry):
        for odd in range(2):
            f = 2 * j + odd
            if odd:
                which = jnp.where(jnp.logical_and(is_last, f == rows2 - 1), 3, 1)
            else:
                which = jnp.where(jnp.logical_and(is_first, f == 0), 2, 0)
            for image in range(images):
                acc = dot(v2[image, f], m2[...]) + bias[0:1, :]
                acc = acc + raised(0, image, j + odd, which)
                put(cat2, image, f, acc)
        return carry

    lax.fori_loop(0, rows2 // 2, pair_rows, 0)

    for level, out in ((1, conv3), (2, conv4), (3, conv5)):
        copies[images + level].wait()
        height = out.shape[1]
        lhs = lambda a: flat(cats[level][:, a : a + height])
        acc = dot(lhs(0), sw[level - 1, 0])
        acc = acc + dot(lhs(1), sw[level - 1, 1])
        acc = acc + dot(lhs(2), sw[level - 1, 2])
        acc = acc.reshape(images, -1, channels)
        out[...] = acc.reshape(out.shape)
        for image in range(images):
            note_sums(stats, 2 * (images * (level - 1) + image), acc[image])
    copies[images + 4].wait()


def fine_kernel(ends, cat2, rim2, sw2, above2, below2, coarse_stats, conv2, stats, halo):
    images, rows2, cols2, _ = cat2.shape
    channels = conv2.shape[-1]
    step = 4 if rows2 % 4 == 0 else 2
    stats[2 * images :, :] = coarse_stats[...]
    for image in range(images):
        for side, source in ((0, above2), (1, below2)):
            acc = source[image].astype(F32) + rim2[side, image]
            put(halo, side, image, jnp.where(ends[side] == 1, 0.0, acc))
    for image in range(images):
        total = square = jnp.zeros((8, channels), F32)
        for r in range(0, rows2, step):
            acc = None
            for tap in range(3):
                low, high = r + tap - 1, r + tap - 1 + step
                lhs = cat2[image, max(low, 0) : min(high, rows2)]
                if low < 0:
                    lhs = jnp.concatenate([halo[0, image][None], lhs], 0)
                if high > rows2:
                    lhs = jnp.concatenate([lhs, halo[1, image][None]], 0)
                res = dot(flat(lhs), sw2[tap])
                acc = res if acc is None else acc + res
            conv2[image, r : r + step] = acc.reshape(step, cols2, channels)
            part = acc.reshape(-1, 8, channels)
            total = total + jnp.sum(part, axis=0)
            square = square + jnp.sum(part * part, axis=0)
        stats[2 * image : 2 * image + 1, :] = jnp.sum(total, axis=0, keepdims=True)
        stats[2 * image + 1 : 2 * image + 2, :] = jnp.sum(square, axis=0, keepdims=True)


def norm_kernel(
    conv2, conv3, conv4, conv5, totals, gain, shift,
    out2, out3, out4, out5,
    s2, s3, s4, s5, sems, *, strips,
):
    channels = conv2.shape[-1]
    width = channels // GROUPS
    row = lax.broadcasted_iota(jnp.int32, (channels, channels), 0) // width
    col = lax.broadcasted_iota(jnp.int32, (channels, channels), 1) // width
    same = jnp.where(row == col, 1.0, 0.0).astype(F32)
    grouped = jnp.dot(
        totals[...], same, precision=lax.Precision.HIGHEST, preferred_element_type=F32
    )
    images = conv2.shape[0]
    copies = []
    levels = ((conv2, s2, out2), (conv3, s3, out3), (conv4, s4, out4), (conv5, s5, out5))
    for level, (conv, stage, out) in enumerate(levels):
        entries = float(conv.shape[1] * strips * conv.shape[2] * width)
        for image in range(images):
            at = 2 * (images * level + image)
            mean = grouped[at : at + 1, :] / entries
            variance = grouped[at + 1 : at + 2, :] / entries - mean * mean
            scale = lax.rsqrt(variance + EPSILON) * gain[level : level + 1, :]
            offset = shift[level : level + 1, :]
            height = conv.shape[1]
            block = min(height, 4)
            for r in range(0, height, block):
                part = flat(conv[image, r : r + block])
                done = ((part - mean) * scale + offset).astype(BF16)
                stage[image, r : r + block] = done.reshape(block, conv.shape[2], channels)
                copy = pltpu.make_async_copy(
                    stage.at[image, pl.ds(r, block)],
                    out.at[image, pl.ds(r, block)],
                    sems.at[len(copies)],
                )
                copy.start()
                copies.append(copy)
    for copy in copies:
        copy.wait()


def total_over(x, axis):
    count = lax.axis_size(axis)
    if count & (count - 1):
        return lax.psum(x, axis)
    step = 1
    while step < count:
        x = x + lax.ppermute(x, axis, [(i, i ^ step) for i in range(count)])
        step *= 2
    return x


def per_device(
    level_two, level_three, level_four, level_five,
    lateral_two, lateral_three, lateral_four, lateral_five,
    lateral_bias, smooth_weight, norm_gain, norm_shift,
):
    position = lax.axis_index("rows")
    strips = lax.axis_size("rows")
    levels = (level_two, level_three, level_four, level_five)
    laterals = (lateral_two, lateral_three, lateral_four, lateral_five)
    levels = tuple(pltpu.with_memory_space_constraint(v, pltpu.HBM) for v in levels)
    laterals = tuple(pltpu.with_memory_space_constraint(v, pltpu.HBM) for v in laterals)
    smooth = pltpu.with_memory_space_constraint(smooth_weight, pltpu.HBM)
    images = level_two.shape[0]
    channels = lateral_two.shape[1]
    widths = tuple(v.shape[2] for v in levels)
    heights = tuple(v.shape[1] for v in levels)
    _, pack = segments(widths[1:])
    hbm = pl.BlockSpec(memory_space=pltpu.HBM)
    vmem = pl.BlockSpec(memory_space=pltpu.VMEM)
    smem = pl.BlockSpec(memory_space=pltpu.SMEM)
    like = lambda v: pltpu.VMEM(v.shape, v.dtype)
    shape = jax.ShapeDtypeStruct
    maps = [shape((images, heights[k], widths[k], channels), F32) for k in range(4)]
    packed = shape((images, pack, channels), BF16)
    packed2 = shape((images, widths[0], channels), BF16)
    table = lambda k: shape((4, widths[k], 2 * widths[k + 1]), BF16)
    lat3, lat4, lat5, downward, upward, downward2, upward2, *tables = pl.pallas_call(
        lateral_kernel,
        out_shape=(maps[1], maps[2], maps[3], packed, packed, packed2, packed2)
        + (table(0), table(1), table(2)),
        in_specs=[hbm] * 9,
        out_specs=[vmem] * 10,
        scratch_shapes=[
            pltpu.VMEM((2, images) + level_two.shape[2:], level_two.dtype),
            like(level_three), like(level_four), like(level_five),
            like(lateral_two), like(lateral_three), like(lateral_four), like(lateral_five),
            like(lateral_bias), pltpu.SemaphoreType.DMA((10,)),
        ],
        compiler_params=pltpu.CompilerParams(vmem_limit_bytes=20 * MIB),
        name="laterals",
    )(*levels, *laterals, pltpu.with_memory_space_constraint(lateral_bias, pltpu.HBM))
    ends = strips - 1
    from_above = lambda v: lax.ppermute(v, "rows", [(i, i + 1) for i in range(ends)])
    from_below = lambda v: lax.ppermute(v, "rows", [(i + 1, i) for i in range(ends)])
    above, below = from_above(downward), from_below(upward)
    above2, below2 = from_above(downward2), from_below(upward2)
    flags = jnp.stack([position == 0, position == ends]).astype(jnp.int32)
    cat = lambda k: pltpu.VMEM((images, heights[k] + 2, widths[k], 3 * channels), BF16)
    conv3, conv4, conv5, coarse_stats, cat2, rim2, sw2 = pl.pallas_call(
        coarse_kernel,
        out_shape=(
            maps[1], maps[2], maps[3], shape((6 * images, channels), F32),
            shape((images, heights[0], widths[0], 3 * channels), BF16),
            shape((2, images, widths[0], channels), F32),
            shape(smooth_weight.shape[1:], BF16),
        ),
        in_specs=[smem, hbm, hbm] + [vmem] * 9 + [hbm],
        out_specs=[vmem] * 7,
        scratch_shapes=[
            like(level_two), like(lateral_two),
            pltpu.VMEM((3,) + smooth_weight.shape[1:], BF16),
            cat(1), cat(2), cat(3),
            pltpu.SemaphoreType.DMA((5 + images,)),
        ],
        compiler_params=pltpu.CompilerParams(vmem_limit_bytes=24 * MIB),
        name="merge_coarse",
    )(flags, levels[0], laterals[0], lateral_bias, lat3, lat4, lat5, *tables, above, below, smooth)
    conv2, stats = pl.pallas_call(
        fine_kernel,
        out_shape=(maps[0], shape((8 * images, channels), F32)),
        in_specs=[smem] + [vmem] * 6,
        out_specs=[vmem] * 2,
        scratch_shapes=[pltpu.VMEM((2, images, widths[0], 3 * channels), BF16)],
        compiler_params=pltpu.CompilerParams(vmem_limit_bytes=24 * MIB),
        name="conv_fine",
    )(flags, cat2, rim2, sw2, above2, below2, coarse_stats)
    convs = (conv2, conv3, conv4, conv5)
    totals = total_over(stats, "rows")
    outs = [jax.ShapeDtypeStruct(m.shape, BF16) for m in maps]
    count = images * sum(h // min(h, 4) for h in heights)
    return tuple(
        pl.pallas_call(
            functools.partial(norm_kernel, strips=strips),
            out_shape=tuple(outs),
            in_specs=[vmem] * 7,
            out_specs=[hbm] * 4,
            scratch_shapes=[like(o) for o in outs] + [pltpu.SemaphoreType.DMA((count,))],
            compiler_params=pltpu.CompilerParams(vmem_limit_bytes=20 * MIB),
            name="normalize",
        )(*convs, totals, norm_gain, norm_shift)
    )


def solution(mesh):
    split = P("batch", "rows", None, None)
    return jax.shard_map(
        per_device,
        mesh=mesh,
        in_specs=(split,) * 4 + (P(),) * 8,
        out_specs=(split,) * 4,
        check_vma=False,
    )
```
